32 devices in a mesh: batch: 2 (over x), col: 4 (over z), row: 4 (over y, core).
Axes of the slice: x: 2, y: 2, z: 4, core: 2. Of those that a mesh axis runs over, the one named last changes fastest.
Arguments:
- d_inv: bfloat16 [384, 256, 256], P(('batch', 'row')), parts along dimension 0
- l_blk: bfloat16 [384, 256, 256], P(('batch', 'row')), parts along dimension 0
- u_blk: bfloat16 [384, 256, 256], P(('batch', 'row')), parts along dimension 0
- rhs_blk: float32 [384, 256, 512], P(('batch', 'row'), None, 'col'), parts along dimension 0
- x_init: float32 [384, 256, 512], P(('batch', 'row'), None, 'col'), parts along dimension 0
Outputs:
- output: float32 [384, 256, 512], P(('batch', 'row'), None, 'col'), parts along dimension 0
There are 2 independent parts. The reference program is written for one: setup_inputs(seed, part) draws one part's arguments, and reference() takes and returns one part's arrays. A program takes and returns all parts, laid end to end along the dimension named above; each array names one.
All inputs are finite; a program needn't handle non-finite values.
Results may differ from the reference program's by a relative error of at most 0.0117393.
Values are sent between devices in bfloat16 or wider.
A program may use at most 1 GiB of HBM per device.

```python
import jax
import jax.numpy as jnp
from jax import lax

BLOCK_ROWS = 192
BLOCK_SIZE = 256
RHS_COLS = 512
SWEEPS = 4


def setup_inputs(seed: int = 0, part: int = 0) -> dict:
    base_key = jax.random.fold_in(jax.random.key(seed), part)
    k_d, k_l, k_u, k_f, k_x = jax.random.split(base_key, 5)
    fan_scale = BLOCK_SIZE ** -0.5
    mat_shape = (BLOCK_ROWS, BLOCK_SIZE, BLOCK_SIZE)
    vec_shape = (BLOCK_ROWS, BLOCK_SIZE, RHS_COLS)
    ident_mat = jnp.eye(BLOCK_SIZE, dtype=jnp.float32)
    row_ids = jnp.arange(BLOCK_ROWS)
    l_mask = (row_ids > 0).astype(jnp.float32)[:, None, None]
    u_mask = (row_ids < BLOCK_ROWS - 1).astype(jnp.float32)[:, None, None]
    d_inv = ident_mat + 0.3 * fan_scale * jax.random.normal(k_d, mat_shape, jnp.float32)
    l_blk = 0.6 * fan_scale * jax.random.normal(k_l, mat_shape, jnp.float32) * l_mask
    u_blk = 0.45 * fan_scale * jax.random.normal(k_u, mat_shape, jnp.float32) * u_mask
    rhs_blk = jax.random.normal(k_f, vec_shape, jnp.float32)
    x_init = jax.random.normal(k_x, vec_shape, jnp.float32)
    return {"d_inv": d_inv.astype(jnp.bfloat16), "l_blk": l_blk.astype(jnp.bfloat16), "u_blk": u_blk.astype(jnp.bfloat16), "rhs_blk": rhs_blk, "x_init": x_init}


def reference(d_inv, l_blk, u_blk, rhs_blk, x_init):
    zero_blk = jnp.zeros((BLOCK_SIZE, RHS_COLS), jnp.float32)

    def row_step(x_left, row_in):
        d_i, l_i, u_i, f_i, x_right = row_in
        t_i = (f_i
               - jnp.dot(l_i, x_left.astype(jnp.bfloat16), preferred_element_type=jnp.float32)
               - jnp.dot(u_i, x_right.astype(jnp.bfloat16), preferred_element_type=jnp.float32))
        x_i = jnp.dot(d_i, t_i.astype(jnp.bfloat16), preferred_element_type=jnp.float32)
        return x_i, x_i

    def one_sweep(x_old, unused):
        x_right = jnp.concatenate([x_old[1:], zero_blk[None]], axis=0)
        _, x_new = lax.scan(row_step, zero_blk, (d_inv, l_blk, u_blk, rhs_blk, x_right))
        return x_new, None

    x_final, _ = lax.scan(one_sweep, x_init, None, length=SWEEPS)
    return x_final
```

```python
import jax
import jax.numpy as jnp
from jax import lax
from jax.experimental import pallas as pl
from jax.experimental.pallas import tpu as pltpu
from jax.sharding import PartitionSpec as P

SWEEPS = 4
GHOST = SWEEPS - 1
LEAD = 2 * SWEEPS - 1
UNROLL = 10
RING = 10
MESH = pl.DeviceIdType.MESH
ORDER = (1, 2, 3, 4)
BF16, F32 = jnp.bfloat16, jnp.float32


def n_ok(name, ring):
    return ring or name != "x"


def dot(a, b):
    return jnp.dot(a, b, preferred_element_type=F32)


def make_kernel(n_dev, n_rows, cols):
    last_row = n_rows - 1
    trips = (n_rows - LEAD - 1) // UNROLL
    main_end = LEAD + trips * UNROLL
    end = n_rows + LEAD
    first = LEAD + 1
    chunks = [(0, 1), (1, 1), (2, 2), (4, first - 4)]
    m0 = len(chunks)
    chunks += [(first + UNROLL * b, UNROLL) for b in range(trips)]
    assert first + UNROLL * trips == n_rows and UNROLL % RING == 0
    ghost = len(chunks)

    def kernel(d_hbm, l_hbm, u_hbm, f_hbm, x_hbm, o_hbm,
               l_all, d_all, u_all, f_raw, x_raw, f_all, x_all, l_ring, d_ring, u_ring, f_ring, out, now, recv, send,
               sem_l, sem_d, sem_u, sem_f, sem_x, sem_o, sem_g, sem_s, sem_r):
        me = lax.axis_index("row")
        arrays = {"l": (l_hbm, l_all, sem_l), "d": (d_hbm, d_all, sem_d), "u": (u_hbm, u_all, sem_u),
                  "f": (f_hbm, f_raw, sem_f), "x": (x_hbm, x_raw, sem_x)}

        def chunk(name, c, start=None, size=None):
            hbm, vmem, sem = arrays[name]
            if start is None:
                start, size = chunks[c]
            rows = pl.ds(start, size)
            return pltpu.make_async_copy(hbm.at[rows], vmem.at[rows], sem.at[c])

        for c in range(ghost):
            for name in "uxdfl":
                chunk(name, c).start()

        def ghost_rows(name):
            return GHOST + 1 if name == "x" else GHOST

        def ghost_copy(i, name):
            hbm, vmem, sem = arrays[name]
            n = ghost_rows(name)
            return pltpu.make_async_remote_copy(
                src_ref=hbm.at[pl.ds(0, n)], dst_ref=vmem.at[pl.ds(n_rows, n)], send_sem=sem_g.at[i],
                recv_sem=sem.at[ghost], device_id={"row": me - 1}, device_id_type=MESH)

        def ghost_local(name):
            hbm, vmem, sem = arrays[name]
            n = ghost_rows(name)
            return pltpu.make_async_copy(hbm.at[pl.ds(0, n)], vmem.at[pl.ds(n_rows, n)], sem.at[ghost])

        def ghost_wait(name):
            ghost_local(name).wait()

        barrier = pltpu.get_barrier_semaphore()

        @pl.when(me > 0)
        def _():
            pl.semaphore_signal(barrier, inc=1, device_id={"row": me - 1}, device_id_type=MESH)

        @pl.when(me < n_dev - 1)
        def _():
            pl.semaphore_signal(barrier, inc=1, device_id={"row": me + 1}, device_id_type=MESH)

        pl.semaphore_wait(barrier, jnp.where(me > 0, 1, 0) + jnp.where(me < n_dev - 1, 1, 0))

        @pl.when(me > 0)
        def _():
            for i, name in enumerate("xuldf"):
                ghost_copy(i, name).start()

        @pl.when(me == n_dev - 1)
        def _():
            for name in "xuldf":
                ghost_local(name).start()

        def boundary(k):
            return pltpu.make_async_remote_copy(
                src_ref=send.at[k], dst_ref=recv.at[k], send_sem=sem_s.at[k], recv_sem=sem_r.at[k],
                device_id={"row": me + 1}, device_id_type=MESH)

        def out_copy(i, start, size):
            rows = pl.ds(start, size)
            return pltpu.make_async_copy(out.at[rows], o_hbm.at[rows], sem_o.at[i])

        def run(ring):
            def where(base, p):
                return p if base is None else base + (p - LEAD)

            def slot(base, r):
                return r % RING if ring else where(base, r)

            big = {"l": l_all, "d": d_all, "u": u_all}
            prep_to = {"l": l_ring, "d": d_ring, "u": u_ring, "f": f_ring} if ring else dict(big, f=f_all)

            def prep(name, base, r):
                at = where(base, r)
                if name == "x":
                    x_all[at] = x_raw[at].astype(BF16).T
                elif name == "f":
                    prep_to["f"][slot(base, r)] = f_raw[at].T
                else:
                    prep_to[name][slot(base, r)] = big[name][at].T

            def active(k, s):
                return 0 <= s - 2 * (k - 1) <= last_row + SWEEPS - k

            def mat(name, base, r):
                return prep_to[name][slot(base, r)]

            def period(x, p, base=None):
                x = dict(x)
                if base is None and p % 2 == 0 and p < 2 * SWEEPS and not ring:
                    k = p // 2 + 1
                    boundary(k - 1).wait_recv()
                    x[k] = recv[k - 1]
                new = {}
                for k in ORDER:
                    if not active(k, p):
                        continue
                    r = p - 2 * (k - 1)
                    if k == 1:
                        right = x_all[where(base, r + 1)]
                    else:
                        right = x[k - 1]
                        if base is None and r == last_row:
                            right = jnp.where(me < n_dev - 1, right, jnp.zeros_like(right))
                    s = dot(right, mat("u", base, r))
                    if k in x:
                        s = s + dot(x[k], mat("l", base, r))
                    t = (prep_to["f"][slot(base, r)] - s).astype(BF16)
                    val = dot(t, mat("d", base, r))
                    new[k] = val.astype(BF16)
                    if k == SWEEPS:
                        out[where(base, r)] = val.T
                    if base is None and r == last_row:
                        send[k - 1] = new[k]

                        @pl.when(me < n_dev - 1)
                        def _():
                            boundary(k - 1).start()
                return new

            def step_preps(p):
                return [(n, p + 1) for n in "ldf"] + [("u", p + 2), ("x", p + 3)]

            waited = set()

            def need(name, r):
                c = max(i for i, (start, _) in enumerate(chunks) if start <= r)
                if (name, c) not in waited:
                    waited.add((name, c))
                    chunk(name, c).wait()

            if ring:
                waited.add(("x", 0))
                chunk("x", 0).wait()
                chunk("l", 0).wait()
                waited.add(("l", 0))
                for name, r in (("u", 0), ("x", 1), ("d", 0), ("f", 0), ("u", 1), ("x", 2)):
                    need(name, r)
                    prep(name, None, r)
            else:
                for c in range(m0):
                    for name in "uxdfl":
                        chunk(name, c).wait()
                for r in range(first):
                    for name in "uxdfl":
                        prep(name, None, r)

                def prepare(b, carry):
                    start = first + UNROLL * b
                    for name in "uxdfl":
                        chunk(name, m0 + b, start, UNROLL).wait()

                    def pair(i, carry):
                        for j in range(2):
                            for name in "uxdfl":
                                prep(name, start + 2 * i, LEAD + j)
                        return carry
                    return lax.fori_loop(0, UNROLL // 2, pair, carry)
                lax.fori_loop(0, trips, prepare, 0)
                ghost_wait("x")
                for r in range(n_rows, n_rows + GHOST + 1):
                    prep("x", None, r)

            def keep(x):
                for k in x:
                    now[k - 1] = x[k]

            def load():
                return {k: now[k - 1] for k in range(1, SWEEPS + 1)}

            x = {}
            for p in range(LEAD):
                for name, r in step_preps(p) if ring else ():
                    need(name, r)
                    prep(name, None, r)
                x = period(x, p)
            keep(x)
            out_copy(trips + 2, 0, 1).start()

            def trip(b, carry):
                base = LEAD + UNROLL * b
                if ring:
                    for name in "ldf":
                        chunk(name, m0 + b, first + UNROLL * b, UNROLL).wait()

                    @pl.when(b < trips - 1)
                    def _():
                        for name in "ux":
                            chunk(name, m0 + b + 1, first + UNROLL * (b + 1), UNROLL).wait()

                    @pl.when(b == trips - 1)
                    def _():
                        for name in "ux":
                            ghost_wait(name)
                x = load()
                for j in range(UNROLL):
                    p = LEAD + j
                    for name, r in step_preps(p) if ring else ():
                        prep(name, base, r)
                    x = period(x, p, base)
                keep(x)
                out_copy(b, 1 + UNROLL * b, UNROLL).start()
                return carry
            lax.fori_loop(0, trips, trip, 0)

            for name in "ldf" if ring else "uldf":
                ghost_wait(name)
            if not ring:
                prep("u", None, n_rows)
            x = load()
            for p in range(main_end, end - 1):
                for name, r in step_preps(p):
                    if n_rows <= r < n_rows + GHOST and (n_ok(name, ring)) or (ring and name == "x" and r == n_rows + GHOST):
                        prep(name, None, r)
                x = {**x, **period(x, p)}
                if p == end - 3:
                    out_copy(trips, 1 + UNROLL * trips, n_rows - UNROLL * trips - 2).start()
            out_copy(trips + 1, last_row, 1).start()

        @pl.when(me == 0)
        def _():
            run(True)

        @pl.when(me > 0)
        def _():
            run(False)

        @pl.when(me < n_dev - 1)
        def _():
            for k in range(SWEEPS):
                boundary(k).wait_send()

        @pl.when(me > 0)
        def _():
            for i, name in enumerate("xuldf"):
                ghost_copy(i, name).wait_send()
        for b in range(trips):
            out_copy(b, 1 + UNROLL * b, UNROLL).wait()
        out_copy(trips, 1 + UNROLL * trips, n_rows - UNROLL * trips - 2).wait()
        out_copy(trips + 2, 0, 1).wait()
        out_copy(trips + 1, last_row, 1).wait()

    def call(d_inv, l_blk, u_blk, rhs_blk, x_init):
        size = d_inv.shape[-1]
        ext = n_rows + GHOST
        dma = pltpu.SemaphoreType.DMA
        mat = lambda n: pltpu.VMEM((n, size, size), BF16)
        vec_t = lambda n, t: pltpu.VMEM((n, cols, size), t)
        vec = lambda n: pltpu.VMEM((n, size, cols), F32)
        return pl.pallas_call(
            kernel,
            out_shape=jax.ShapeDtypeStruct((n_rows, size, cols), F32),
            in_specs=[pl.BlockSpec(memory_space=pltpu.HBM)] * 5,
            out_specs=pl.BlockSpec(memory_space=pltpu.HBM),
            scratch_shapes=[
                mat(ext), mat(ext), mat(ext), vec(ext), vec(ext + 1), vec_t(ext, F32), vec_t(ext + 1, BF16),
                mat(RING), mat(RING), mat(RING), vec_t(RING, F32),
                vec(n_rows), vec_t(SWEEPS, BF16), vec_t(SWEEPS, BF16), vec_t(SWEEPS, BF16),
                *[dma((ghost + 1,)) for _ in range(5)], dma((trips + 3,)), dma((5,)), dma((SWEEPS,)), dma((SWEEPS,)),
            ],
            compiler_params=pltpu.CompilerParams(
                collective_id=0, has_side_effects=True, vmem_limit_bytes=67_000_000),
        )(d_inv, l_blk, u_blk, rhs_blk, x_init)

    return call


def solution(mesh):
    mat_spec = P(("batch", "row"), None, None)
    vec_spec = P(("batch", "row"), None, "col")
    n_dev = mesh.shape["row"]

    def device_fn(d_inv, l_blk, u_blk, rhs_blk, x_init):
        return make_kernel(n_dev, rhs_blk.shape[0], rhs_blk.shape[2])(d_inv, l_blk, u_blk, rhs_blk, x_init)

    return jax.shard_map(device_fn, mesh=mesh, in_specs=(mat_spec, mat_spec, mat_spec, vec_spec, vec_spec), out_specs=vec_spec, check_vma=False)
```

```python
import jax
import jax.numpy as jnp
from jax import lax
from jax.experimental import pallas as pl
from jax.experimental.pallas import tpu as pltpu
from jax.sharding import PartitionSpec as P

SWEEPS = 4
GHOST = SWEEPS - 1
LEAD = 2 * SWEEPS - 1
UNROLL = 10
RING = 10
MESH = pl.DeviceIdType.MESH
BF16, F32 = jnp.bfloat16, jnp.float32


def dot(a, b):
    return jnp.dot(a, b, preferred_element_type=F32)


def make_kernel(n_dev, n_rows, cols):
    last_row = n_rows - 1
    trips = (n_rows - LEAD - 1) // UNROLL
    main_end = LEAD + trips * UNROLL
    end = n_rows + LEAD
    first = LEAD + 1
    chunks = [(0, 1), (1, 1), (2, 2), (4, first - 4)]
    m0 = len(chunks)
    chunks += [(first + UNROLL * b, UNROLL) for b in range(trips)]
    assert first + UNROLL * trips == n_rows and UNROLL % RING == 0
    ghost = len(chunks)

    def kernel(d_hbm, l_hbm, u_hbm, f_hbm, x_hbm, o_hbm,
               l_all, d_all, u_all, f_raw, x_raw, f_all, x_all, l_ring, d_ring, u_ring, f_ring, out, hold, recv, send,
               sem_l, sem_d, sem_u, sem_f, sem_x, sem_o, sem_g, sem_s, sem_r):
        me = lax.axis_index("row")
        arrays = {"l": (l_hbm, l_all, sem_l), "d": (d_hbm, d_all, sem_d), "u": (u_hbm, u_all, sem_u),
                  "f": (f_hbm, f_raw, sem_f), "x": (x_hbm, x_raw, sem_x)}

        def chunk(name, c, start=None, size=None):
            hbm, vmem, sem = arrays[name]
            if start is None:
                start, size = chunks[c]
            rows = pl.ds(start, size)
            return pltpu.make_async_copy(hbm.at[rows], vmem.at[rows], sem.at[c])

        for c in range(ghost):
            for name in "uxdfl":
                chunk(name, c).start()

        def ghost_rows(name):
            return GHOST + 1 if name == "x" else GHOST

        def ghost_copy(i, name):
            hbm, vmem, sem = arrays[name]
            n = ghost_rows(name)
            return pltpu.make_async_remote_copy(
                src_ref=hbm.at[pl.ds(0, n)], dst_ref=vmem.at[pl.ds(n_rows, n)], send_sem=sem_g.at[i],
                recv_sem=sem.at[ghost], device_id={"row": me - 1}, device_id_type=MESH)

        def ghost_local(name):
            hbm, vmem, sem = arrays[name]
            n = ghost_rows(name)
            return pltpu.make_async_copy(hbm.at[pl.ds(0, n)], vmem.at[pl.ds(n_rows, n)], sem.at[ghost])

        def ghost_wait(name):
            ghost_local(name).wait()

        barrier = pltpu.get_barrier_semaphore()

        @pl.when(me > 0)
        def _():
            pl.semaphore_signal(barrier, inc=1, device_id={"row": me - 1}, device_id_type=MESH)

        @pl.when(me < n_dev - 1)
        def _():
            pl.semaphore_signal(barrier, inc=1, device_id={"row": me + 1}, device_id_type=MESH)

        pl.semaphore_wait(barrier, jnp.where(me > 0, 1, 0) + jnp.where(me < n_dev - 1, 1, 0))

        @pl.when(me > 0)
        def _():
            for i, name in enumerate("xuldf"):
                ghost_copy(i, name).start()

        @pl.when(me == n_dev - 1)
        def _():
            for name in "xuldf":
                ghost_local(name).start()

        def boundary(k):
            return pltpu.make_async_remote_copy(
                src_ref=send.at[k], dst_ref=recv.at[k], send_sem=sem_s.at[k], recv_sem=sem_r.at[k],
                device_id={"row": me + 1}, device_id_type=MESH)

        def out_copy(i, start, size):
            rows = pl.ds(start, size)
            return pltpu.make_async_copy(out.at[rows], o_hbm.at[rows], sem_o.at[i])

        def run(ring):
            def where(base, p):
                return p if base is None else base + (p - LEAD)

            def slot(base, r):
                return r % RING if ring else where(base, r)

            big = {"l": l_all, "d": d_all, "u": u_all}
            prep_to = {"l": l_ring, "d": d_ring, "u": u_ring, "f": f_ring} if ring else dict(big, f=f_all)

            def prep(name, base, r):
                at = where(base, r)
                if name == "x":
                    x_all[at] = x_raw[at].astype(BF16).T
                elif name == "f":
                    prep_to["f"][slot(base, r)] = f_raw[at].T
                else:
                    prep_to[name][slot(base, r)] = big[name][at].T

            def active(k, s):
                return 0 <= s - 2 * (k - 1) <= last_row + SWEEPS - k

            def mat(name, base, r):
                return prep_to[name][slot(base, r)]

            def period(live, p, base=None, preps=()):
                x = {}

                def get_x(k):
                    if ("x", k) in live:
                        val = live.pop(("x", k))
                        x[k] = val.astype(BF16)
                        if k == SWEEPS:
                            out[where(base, p - LEAD)] = val.T
                        if base is None and p - 1 - 2 * (k - 1) == last_row:
                            send[k - 1] = x[k]

                            @pl.when(me < n_dev - 1)
                            def _():
                                boundary(k - 1).start()
                    elif base is None and p == 2 * (k - 1) and not ring:
                        boundary(k - 1).wait_recv()
                        x[k] = recv[k - 1]

                def add(k, val):
                    live["t", k] = live["t", k] + val if ("t", k) in live else val

                def mul_l(k):
                    if active(k, p) and not (ring and base is None and p == 2 * (k - 1)):
                        add(k, dot(x[k], mat("l", base, p - 2 * (k - 1))))

                def mul_u(k):
                    if active(k, p):
                        r = p - 2 * (k - 1)
                        val = x[k - 1]
                        if base is None and r == last_row:
                            val = jnp.where(me < n_dev - 1, val, jnp.zeros_like(val))
                        add(k, dot(val, mat("u", base, r)))

                def mul_u1(s):
                    if active(1, s):
                        add(1, dot(x_all[where(base, s + 1)], mat("u", base, s)))

                def mul_d(k, s):
                    if ("t", k) in live:
                        r = s - 2 * (k - 1)
                        t = (prep_to["f"][slot(base, r)] - live.pop(("t", k))).astype(BF16)
                        live["x", k] = dot(t, mat("d", base, r))

                for name, r in preps:
                    prep(name, base, r)
                if ("t", 1) not in live:
                    mul_u1(p)
                get_x(1)
                mul_l(1)
                mul_d(3, p - 1)
                mul_u(2)
                get_x(2)
                mul_l(2)
                mul_u(3)
                mul_d(4, p - 1)
                mul_d(1, p)
                mul_u1(p + 1)
                get_x(3)
                mul_l(3)
                mul_d(2, p)
                mul_u(4)
                get_x(4)
                mul_l(4)

            def step_preps(p):
                return [(n, p + 1) for n in "ldf"] + [("u", p + 2), ("x", p + 3)]

            waited = set()

            def need(name, r):
                c = max(i for i, (start, _) in enumerate(chunks) if start <= r)
                if (name, c) not in waited:
                    waited.add((name, c))
                    chunk(name, c).wait()

            if ring:
                waited.add(("x", 0))
                chunk("x", 0).wait()
                chunk("l", 0).wait()
                waited.add(("l", 0))
                for name, r in (("u", 0), ("x", 1), ("d", 0), ("f", 0), ("u", 1), ("x", 2)):
                    need(name, r)
                    prep(name, None, r)
            else:
                for c in range(m0):
                    for name in "uxdfl":
                        chunk(name, c).wait()
                for r in range(first):
                    for name in "uxdfl":
                        prep(name, None, r)

                def prepare(b, carry):
                    start = first + UNROLL * b
                    for name in "uxdfl":
                        chunk(name, m0 + b, start, UNROLL).wait()

                    def pair(i, carry):
                        for j in range(2):
                            for name in "uxdfl":
                                prep(name, start + 2 * i, LEAD + j)
                        return carry
                    return lax.fori_loop(0, UNROLL // 2, pair, carry)
                lax.fori_loop(0, trips, prepare, 0)
                ghost_wait("x")
                for r in range(n_rows, n_rows + GHOST + 1):
                    prep("x", None, r)

            def keep(live):
                for k in (1, 2):
                    hold[k - 1] = live["x", k]
                for k in (1, 3, 4):
                    hold[1 + max(k - 1, 1)] = live["t", k]

            def load():
                live = {("x", k): hold[k - 1] for k in (1, 2)}
                return {**live, **{("t", k): hold[1 + max(k - 1, 1)] for k in (1, 3, 4)}}

            live = {}
            for p in range(LEAD):
                preps = step_preps(p) if ring else ()
                for name, r in preps:
                    need(name, r)
                period(live, p, None, preps)
            keep(live)

            def trip(b, carry):
                base = LEAD + UNROLL * b
                if ring:
                    for name in "ldf":
                        chunk(name, m0 + b, first + UNROLL * b, UNROLL).wait()

                    @pl.when(b < trips - 1)
                    def _():
                        for name in "ux":
                            chunk(name, m0 + b + 1, first + UNROLL * (b + 1), UNROLL).wait()

                    @pl.when(b == trips - 1)
                    def _():
                        for name in "ux":
                            ghost_wait(name)
                live = load()
                for j in range(UNROLL):
                    p = LEAD + j
                    period(live, p, base, step_preps(p) if ring else ())
                keep(live)
                out_copy(b, UNROLL * b, UNROLL).start()
                return carry
            lax.fori_loop(0, trips, trip, 0)

            for name in "ldf" if ring else "uldf":
                ghost_wait(name)
            live = load()
            if not ring:
                prep("u", None, n_rows)
            for p in range(main_end, end):
                preps = [(n, r) for n, r in step_preps(p) if n_rows <= r < n_rows + GHOST and (n != "x" or ring)]
                if ring and p + 3 == n_rows + GHOST:
                    preps.append(("x", p + 3))
                period(live, p, None, preps)
                if p == end - 2:
                    out_copy(trips, UNROLL * trips, n_rows - UNROLL * trips - 1).start()
            out_copy(trips + 1, last_row, 1).start()

        @pl.when(me == 0)
        def _():
            run(True)

        @pl.when(me > 0)
        def _():
            run(False)

        @pl.when(me < n_dev - 1)
        def _():
            for k in range(SWEEPS):
                boundary(k).wait_send()

        @pl.when(me > 0)
        def _():
            for i, name in enumerate("xuldf"):
                ghost_copy(i, name).wait_send()
        for b in range(trips):
            out_copy(b, UNROLL * b, UNROLL).wait()
        out_copy(trips, UNROLL * trips, n_rows - UNROLL * trips - 1).wait()
        out_copy(trips + 1, last_row, 1).wait()

    def call(d_inv, l_blk, u_blk, rhs_blk, x_init):
        size = d_inv.shape[-1]
        ext = n_rows + GHOST
        dma = pltpu.SemaphoreType.DMA
        mat = lambda n: pltpu.VMEM((n, size, size), BF16)
        vec_t = lambda n, t: pltpu.VMEM((n, cols, size), t)
        vec = lambda n: pltpu.VMEM((n, size, cols), F32)
        return pl.pallas_call(
            kernel,
            out_shape=jax.ShapeDtypeStruct((n_rows, size, cols), F32),
            in_specs=[pl.BlockSpec(memory_space=pltpu.HBM)] * 5,
            out_specs=pl.BlockSpec(memory_space=pltpu.HBM),
            scratch_shapes=[
                mat(ext), mat(ext), mat(ext), vec(ext), vec(ext + 1), vec_t(ext, F32), vec_t(ext + 1, BF16),
                mat(RING), mat(RING), mat(RING), vec_t(RING, F32),
                vec(n_rows), vec_t(5, F32), vec_t(SWEEPS, BF16), vec_t(SWEEPS, BF16),
                *[dma((ghost + 1,)) for _ in range(5)], dma((trips + 2,)), dma((5,)), dma((SWEEPS,)), dma((SWEEPS,)),
            ],
            compiler_params=pltpu.CompilerParams(
                collective_id=0, has_side_effects=True, vmem_limit_bytes=67_000_000),
        )(d_inv, l_blk, u_blk, rhs_blk, x_init)

    return call


def solution(mesh):
    mat_spec = P(("batch", "row"), None, None)
    vec_spec = P(("batch", "row"), None, "col")
    n_dev = mesh.shape["row"]

    def device_fn(d_inv, l_blk, u_blk, rhs_blk, x_init):
        return make_kernel(n_dev, rhs_blk.shape[0], rhs_blk.shape[2])(d_inv, l_blk, u_blk, rhs_blk, x_init)

    return jax.shard_map(device_fn, mesh=mesh, in_specs=(mat_spec, mat_spec, mat_spec, vec_spec, vec_spec), out_specs=vec_spec, check_vma=False)
```

```python
import jax
import jax.numpy as jnp
from jax import lax
from jax.experimental import pallas as pl
from jax.experimental.pallas import tpu as pltpu
from jax.sharding import PartitionSpec as P

SWEEPS = 4
GHOST = SWEEPS - 1
LEAD = 2 * SWEEPS - 1
UNROLL = 10
RING = 10
MESH = pl.DeviceIdType.MESH
BF16, F32 = jnp.bfloat16, jnp.float32


def dot(a, b):
    return jnp.dot(a, b, preferred_element_type=F32)


def make_kernel(n_dev, n_rows, cols):
    last_row = n_rows - 1
    trips = (n_rows - LEAD - 1) // UNROLL
    main_end = LEAD + trips * UNROLL
    end = n_rows + LEAD
    first = LEAD + 1
    chunks = [(0, 1), (1, 1), (2, 2), (4, first - 4)]
    m0 = len(chunks)
    chunks += [(first + UNROLL * b, UNROLL) for b in range(trips)]
    assert first + UNROLL * trips == n_rows and UNROLL % RING == 0
    ghost = len(chunks)

    def kernel(d_hbm, l_hbm, u_hbm, f_hbm, x_hbm, out,
               l_all, d_all, u_all, f_raw, x_raw, f_all, x_all, l_ring, d_ring, u_ring, f_ring, hold, recv, send,
               sem_l, sem_d, sem_u, sem_f, sem_x, sem_g, sem_s, sem_r):
        me = lax.axis_index("row")
        arrays = {"l": (l_hbm, l_all, sem_l), "d": (d_hbm, d_all, sem_d), "u": (u_hbm, u_all, sem_u),
                  "f": (f_hbm, f_raw, sem_f), "x": (x_hbm, x_raw, sem_x)}

        def chunk(name, c, start=None, size=None):
            hbm, vmem, sem = arrays[name]
            if start is None:
                start, size = chunks[c]
            rows = pl.ds(start, size)
            return pltpu.make_async_copy(hbm.at[rows], vmem.at[rows], sem.at[c])

        for c in range(ghost):
            for name in "uxdfl":
                chunk(name, c).start()

        def ghost_rows(name):
            return GHOST + 1 if name == "x" else GHOST

        def ghost_copy(i, name):
            hbm, vmem, sem = arrays[name]
            n = ghost_rows(name)
            return pltpu.make_async_remote_copy(
                src_ref=hbm.at[pl.ds(0, n)], dst_ref=vmem.at[pl.ds(n_rows, n)], send_sem=sem_g.at[i],
                recv_sem=sem.at[ghost], device_id={"row": me - 1}, device_id_type=MESH)

        def ghost_local(name):
            hbm, vmem, sem = arrays[name]
            n = ghost_rows(name)
            return pltpu.make_async_copy(hbm.at[pl.ds(0, n)], vmem.at[pl.ds(n_rows, n)], sem.at[ghost])

        def ghost_wait(name):
            ghost_local(name).wait()

        barrier = pltpu.get_barrier_semaphore()

        @pl.when(me > 0)
        def _():
            pl.semaphore_signal(barrier, inc=1, device_id={"row": me - 1}, device_id_type=MESH)

        @pl.when(me < n_dev - 1)
        def _():
            pl.semaphore_signal(barrier, inc=1, device_id={"row": me + 1}, device_id_type=MESH)

        pl.semaphore_wait(barrier, jnp.where(me > 0, 1, 0) + jnp.where(me < n_dev - 1, 1, 0))

        @pl.when(me > 0)
        def _():
            for i, name in enumerate("xuldf"):
                ghost_copy(i, name).start()

        @pl.when(me == n_dev - 1)
        def _():
            for name in "xuldf":
                ghost_local(name).start()

        def boundary(k):
            return pltpu.make_async_remote_copy(
                src_ref=send.at[k], dst_ref=recv.at[k], send_sem=sem_s.at[k], recv_sem=sem_r.at[k],
                device_id={"row": me + 1}, device_id_type=MESH)

        def run(ring):
            def where(base, p):
                return p if base is None else base + (p - LEAD)

            def slot(base, r):
                return r % RING if ring else where(base, r)

            big = {"l": l_all, "d": d_all, "u": u_all}
            prep_to = {"l": l_ring, "d": d_ring, "u": u_ring, "f": f_ring} if ring else dict(big, f=f_all)

            def prep(name, base, r):
                at = where(base, r)
                if name == "x":
                    x_all[at] = x_raw[at].astype(BF16).T
                elif name == "f":
                    prep_to["f"][slot(base, r)] = f_raw[at].T
                else:
                    prep_to[name][slot(base, r)] = big[name][at].T

            def active(k, s):
                return 0 <= s - 2 * (k - 1) <= last_row + SWEEPS - k

            def mat(name, base, r):
                return prep_to[name][slot(base, r)]

            def period(live, p, base=None, preps=()):
                x = {}

                def get_x(k):
                    if ("x", k) in live:
                        val = live.pop(("x", k))
                        x[k] = val.astype(BF16)
                        if k == SWEEPS:
                            out[where(base, p - LEAD)] = val.T
                        if base is None and p - 1 - 2 * (k - 1) == last_row:
                            send[k - 1] = x[k]

                            @pl.when(me < n_dev - 1)
                            def _():
                                boundary(k - 1).start()
                    elif base is None and p == 2 * (k - 1) and not ring:
                        boundary(k - 1).wait_recv()
                        x[k] = recv[k - 1]

                def add(k, val):
                    live["t", k] = live["t", k] + val if ("t", k) in live else val

                def mul_l(k):
                    if active(k, p) and not (ring and base is None and p == 2 * (k - 1)):
                        add(k, dot(x[k], mat("l", base, p - 2 * (k - 1))))

                def mul_u(k):
                    if active(k, p):
                        r = p - 2 * (k - 1)
                        val = x[k - 1]
                        if base is None and r == last_row:
                            val = jnp.where(me < n_dev - 1, val, jnp.zeros_like(val))
                        add(k, dot(val, mat("u", base, r)))

                def mul_u1(s):
                    if active(1, s):
                        add(1, dot(x_all[where(base, s + 1)], mat("u", base, s)))

                def mul_d(k, s):
                    if ("t", k) in live:
                        r = s - 2 * (k - 1)
                        t = (prep_to["f"][slot(base, r)] - live.pop(("t", k))).astype(BF16)
                        live["x", k] = dot(t, mat("d", base, r))

                for name, r in preps:
                    prep(name, base, r)
                if ("t", 1) not in live:
                    mul_u1(p)
                get_x(1)
                mul_l(1)
                mul_d(3, p - 1)
                mul_u(2)
                get_x(2)
                mul_l(2)
                mul_u(3)
                mul_d(4, p - 1)
                mul_d(1, p)
                mul_u1(p + 1)
                get_x(3)
                mul_l(3)
                mul_d(2, p)
                mul_u(4)
                get_x(4)
                mul_l(4)

            def step_preps(p):
                return [(n, p + 1) for n in "ldf"] + [("u", p + 2), ("x", p + 3)]

            waited = set()

            def need(name, r):
                c = max(i for i, (start, _) in enumerate(chunks) if start <= r)
                if (name, c) not in waited:
                    waited.add((name, c))
                    chunk(name, c).wait()

            if ring:
                waited.add(("x", 0))
                chunk("x", 0).wait()
                chunk("l", 0).wait()
                waited.add(("l", 0))
                for name, r in (("u", 0), ("x", 1), ("d", 0), ("f", 0), ("u", 1), ("x", 2)):
                    need(name, r)
                    prep(name, None, r)
            else:
                for c in range(m0):
                    for name in "uxdfl":
                        chunk(name, c).wait()
                for r in range(first):
                    for name in "uxdfl":
                        prep(name, None, r)

                def prepare(b, carry):
                    start = first + UNROLL * b
                    for name in "uxdfl":
                        chunk(name, m0 + b, start, UNROLL).wait()

                    def pair(i, carry):
                        for j in range(2):
                            for name in "uxdfl":
                                prep(name, start + 2 * i, LEAD + j)
                        return carry
                    return lax.fori_loop(0, UNROLL // 2, pair, carry)
                lax.fori_loop(0, trips, prepare, 0)
                ghost_wait("x")
                for r in range(n_rows, n_rows + GHOST + 1):
                    prep("x", None, r)

            def keep(live):
                for k in (1, 2):
                    hold[k - 1] = live["x", k]
                for k in (1, 3, 4):
                    hold[1 + max(k - 1, 1)] = live["t", k]

            def load():
                live = {("x", k): hold[k - 1] for k in (1, 2)}
                return {**live, **{("t", k): hold[1 + max(k - 1, 1)] for k in (1, 3, 4)}}

            live = {}
            for p in range(LEAD):
                preps = step_preps(p) if ring else ()
                for name, r in preps:
                    need(name, r)
                period(live, p, None, preps)
            keep(live)

            def trip(b, carry):
                base = LEAD + UNROLL * b
                if ring:
                    for name in "ldf":
                        chunk(name, m0 + b, first + UNROLL * b, UNROLL).wait()

                    @pl.when(b < trips - 1)
                    def _():
                        for name in "ux":
                            chunk(name, m0 + b + 1, first + UNROLL * (b + 1), UNROLL).wait()

                    @pl.when(b == trips - 1)
                    def _():
                        for name in "ux":
                            ghost_wait(name)
                live = load()
                for j in range(UNROLL):
                    p = LEAD + j
                    period(live, p, base, step_preps(p) if ring else ())
                keep(live)
                return carry
            lax.fori_loop(0, trips, trip, 0)

            for name in "ldf" if ring else "uldf":
                ghost_wait(name)
            live = load()
            if not ring:
                prep("u", None, n_rows)
            for p in range(main_end, end):
                preps = [(n, r) for n, r in step_preps(p) if n_rows <= r < n_rows + GHOST and (n != "x" or ring)]
                if ring and p + 3 == n_rows + GHOST:
                    preps.append(("x", p + 3))
                period(live, p, None, preps)

        @pl.when(me == 0)
        def _():
            run(True)

        @pl.when(me > 0)
        def _():
            run(False)

        @pl.when(me < n_dev - 1)
        def _():
            for k in range(SWEEPS):
                boundary(k).wait_send()

        @pl.when(me > 0)
        def _():
            for i, name in enumerate("xuldf"):
                ghost_copy(i, name).wait_send()

    def call(d_inv, l_blk, u_blk, rhs_blk, x_init):
        size = d_inv.shape[-1]
        ext = n_rows + GHOST
        dma = pltpu.SemaphoreType.DMA
        mat = lambda n: pltpu.VMEM((n, size, size), BF16)
        vec_t = lambda n, t: pltpu.VMEM((n, cols, size), t)
        vec = lambda n: pltpu.VMEM((n, size, cols), F32)
        return pl.pallas_call(
            kernel,
            out_shape=pltpu.VMEM((n_rows, size, cols), F32),
            in_specs=[pl.BlockSpec(memory_space=pltpu.HBM)] * 5,
            out_specs=pl.BlockSpec(memory_space=pltpu.VMEM),
            scratch_shapes=[
                mat(ext), mat(ext), mat(ext), vec(ext), vec(ext + 1), vec_t(ext, F32), vec_t(ext + 1, BF16),
                mat(RING), mat(RING), mat(RING), vec_t(RING, F32),
                vec_t(5, F32), vec_t(SWEEPS, BF16), vec_t(SWEEPS, BF16),
                *[dma((ghost + 1,)) for _ in range(5)], dma((5,)), dma((SWEEPS,)), dma((SWEEPS,)),
            ],
            compiler_params=pltpu.CompilerParams(
                collective_id=0, has_side_effects=True, vmem_limit_bytes=58_000_000),
        )(d_inv, l_blk, u_blk, rhs_blk, x_init)

    return call


def solution(mesh):
    mat_spec = P(("batch", "row"), None, None)
    vec_spec = P(("batch", "row"), None, "col")
    n_dev = mesh.shape["row"]

    def device_fn(d_inv, l_blk, u_blk, rhs_blk, x_init):
        return make_kernel(n_dev, rhs_blk.shape[0], rhs_blk.shape[2])(d_inv, l_blk, u_blk, rhs_blk, x_init)

    return jax.shard_map(device_fn, mesh=mesh, in_specs=(mat_spec, mat_spec, mat_spec, vec_spec, vec_spec), out_specs=vec_spec, check_vma=False)
```

```python
import jax
import jax.numpy as jnp
from jax import lax
from jax.experimental import pallas as pl
from jax.experimental.pallas import tpu as pltpu
from jax.sharding import PartitionSpec as P

SWEEPS = 4
GHOST = SWEEPS - 1
LEAD = 2 * SWEEPS - 1
LEAD_FIRST = LEAD + 10
TRIP_FIRST = 10
TRIP = 20
RING = 10
CHUNKS = (1, 1, 2, 4, 4, 6)
MESH = pl.DeviceIdType.MESH
BF16, F32 = jnp.bfloat16, jnp.float32
NAMES = "uxdfl"


def dot(a, b):
    return jnp.dot(a, b, preferred_element_type=F32)


def make_kernel(n_dev, n_rows, size, cols):
    last_row = n_rows - 1
    end = n_rows + LEAD
    sizes = list(CHUNKS) + [TRIP_FIRST] * ((n_rows - sum(CHUNKS)) // TRIP_FIRST)
    starts = [sum(sizes[:i]) for i in range(len(sizes))]
    assert sum(sizes) == n_rows and sum(CHUNKS) == LEAD_FIRST + 1 and TRIP_FIRST % RING == 0
    ghost = len(sizes)
    trips_first = ghost - len(CHUNKS)
    trips = (n_rows - 1 - LEAD) // TRIP

    def kernel(d_hbm, l_hbm, u_hbm, f_hbm, x_hbm, out,
               ul_all, d_all, f_raw, x_raw, f_all, x_all, ul_ring, d_ring, f_ring, hold, recv, send,
               sem_l, sem_d, sem_u, sem_f, sem_x, sem_g, sem_s, sem_r):
        me = lax.axis_index("row")
        hbm = {"l": l_hbm, "d": d_hbm, "u": u_hbm, "f": f_hbm, "x": x_hbm}
        sems = {"l": sem_l, "d": sem_d, "u": sem_u, "f": sem_f, "x": sem_x}
        half = {"u": pl.ds(0, size), "l": pl.ds(size, size)}

        def landing(name, rows):
            if name in half:
                return ul_all.at[rows, half[name]]
            return {"d": d_all, "f": f_raw, "x": x_raw}[name].at[rows]

        def local(name, c, start, n):
            if name == "x":
                start = start + 1
            rows = pl.ds(start, n)
            return pltpu.make_async_copy(hbm[name].at[rows], landing(name, rows), sems[name].at[c])

        def chunk(name, c):
            last = name == "x" and c == ghost - 1
            return local(name, c, starts[c], sizes[c] - last)

        for c in range(ghost):
            for name in NAMES:
                chunk(name, c).start()

        def ghost_rows(name):
            return GHOST + 1 if name == "x" else GHOST

        def ghost_copy(i, name):
            n = ghost_rows(name)
            return pltpu.make_async_remote_copy(
                src_ref=hbm[name].at[pl.ds(0, n)], dst_ref=landing(name, pl.ds(n_rows, n)), send_sem=sem_g.at[i],
                recv_sem=sems[name].at[ghost], device_id={"row": me - 1}, device_id_type=MESH)

        def ghost_local(name):
            n = ghost_rows(name)
            return pltpu.make_async_copy(
                hbm[name].at[pl.ds(0, n)], landing(name, pl.ds(n_rows, n)), sems[name].at[ghost])

        def ghost_wait(name):
            ghost_local(name).wait()

        barrier = pltpu.get_barrier_semaphore()

        @pl.when(me > 0)
        def _():
            pl.semaphore_signal(barrier, inc=1, device_id={"row": me - 1}, device_id_type=MESH)

        @pl.when(me < n_dev - 1)
        def _():
            pl.semaphore_signal(barrier, inc=1, device_id={"row": me + 1}, device_id_type=MESH)

        pl.semaphore_wait(barrier, jnp.where(me > 0, 1, 0) + jnp.where(me < n_dev - 1, 1, 0))

        @pl.when(me > 0)
        def _():
            for i, name in enumerate("xuldf"):
                ghost_copy(i, name).start()

        @pl.when(me == n_dev - 1)
        def _():
            for name in "xuldf":
                ghost_local(name).start()

        def boundary(k):
            return pltpu.make_async_remote_copy(
                src_ref=send.at[k], dst_ref=recv.at[k], send_sem=sem_s.at[k], recv_sem=sem_r.at[k],
                device_id={"row": me + 1}, device_id_type=MESH)

        def run(ring):
            lead = LEAD_FIRST if ring else LEAD
            per_trip, n_trips = (TRIP_FIRST, trips_first) if ring else (TRIP, trips)
            main_end = lead + per_trip * n_trips
            ul, d, f = (ul_ring, d_ring, f_ring) if ring else (ul_all, d_all, f_all)

            def where(base, p):
                return p if base is None else base + (p - lead)

            def slot(base, r):
                return r % RING if ring else where(base, r)

            def prep(base, r):
                at, to = where(base, r), slot(base, r)
                for name in "ul":
                    ul[to, half[name]] = ul_all[at, half[name]].T
                d[to] = d_all[at].T
                f[to] = f_raw[at].T
                x_all[at + 1] = x_raw[at + 1].astype(BF16).T

            def active(k, s):
                return 0 <= s - 2 * (k - 1) <= last_row + SWEEPS - k

            def period(live, p, base=None):
                x = {}

                def get_x(k):
                    if ("x", k) in live:
                        val = live.pop(("x", k))
                        x[k] = val.astype(BF16)
                        if k == SWEEPS:
                            out[where(base, p - LEAD)] = val.T
                        if base is None and p - 1 - 2 * (k - 1) == last_row:
                            send[k - 1] = x[k]

                            @pl.when(me < n_dev - 1)
                            def _():
                                boundary(k - 1).start()
                    elif base is None and p == 2 * (k - 1) and not ring:
                        boundary(k - 1).wait_recv()
                        x[k] = recv[k - 1]

                def sums(k):
                    get_x(k)
                    if not active(k, p):
                        return
                    r = p - 2 * (k - 1)
                    right = x_all[where(base, r + 1)] if k == 1 else x[k - 1]
                    if base is None and k > 1 and r == last_row:
                        right = jnp.where(me < n_dev - 1, right, jnp.zeros_like(right))
                    if k in x:
                        live["t", k] = dot(jnp.concatenate([right, x[k]], axis=1), ul[slot(base, r)])
                    else:
                        live["t", k] = dot(right, ul[slot(base, r), half["u"]])

                def solve(k, s):
                    if ("t", k) in live:
                        to = slot(base, s - 2 * (k - 1))
                        live["x", k] = dot((f[to] - live.pop(("t", k))).astype(BF16), d[to])

                sums(1)
                sums(2)
                solve(3, p - 1)
                sums(3)
                solve(4, p - 1)
                solve(1, p)
                sums(4)
                solve(2, p)

            carried = (("x", 1), ("x", 2), ("t", 3), ("t", 4))

            def keep(live):
                for i, key in enumerate(carried):
                    hold[i] = live[key]

            def load():
                return {key: hold[i] for i, key in enumerate(carried)}

            if ring:
                waited = set()

                def need(r):
                    c = max(i for i, start in enumerate(starts) if start <= r)
                    if c not in waited:
                        waited.add(c)
                        for name in NAMES:
                            chunk(name, c).wait()

                need(0)
                prep(None, 0)
            else:
                for c in range(1, ghost):
                    for i in ([0, 1] if c == 1 else [c]):
                        for name in NAMES:
                            chunk(name, i).wait()
                    if c == ghost - 1:
                        ghost_wait("x")
                    start = 0 if c == 1 else starts[c]

                    def pair(i, carry, start=start):
                        prep(start + 2 * i, lead)
                        prep(start + 2 * i, lead + 1)
                        return carry
                    lax.fori_loop(0, (starts[c] + sizes[c] - start) // 2, pair, 0)
            live = {}
            for p in range(lead):
                if ring:
                    need(p + 1)
                    prep(None, p + 1)
                period(live, p)
            keep(live)

            def trip(b, carry):
                base = lead + per_trip * b
                if ring:
                    c, start = len(CHUNKS) + b, lead + 1 + per_trip * b
                    for name in "udfl":
                        local(name, c, start, per_trip).wait()

                    @pl.when(b < n_trips - 1)
                    def _():
                        local("x", c, start, per_trip).wait()

                    @pl.when(b == n_trips - 1)
                    def _():
                        chunk("x", ghost - 1).wait()
                        ghost_wait("x")
                live = load()
                for p in range(lead, lead + per_trip):
                    if ring:
                        prep(base, p + 1)
                    period(live, p, base)
                keep(live)
                return carry
            lax.fori_loop(0, n_trips, trip, 0)

            for name in "uldf":
                ghost_wait(name)
            live = load()
            for p in range(main_end, end):
                if n_rows <= p + 1 < n_rows + GHOST:
                    prep(None, p + 1)
                period(live, p)

        @pl.when(me == 0)
        def _():
            run(True)

        @pl.when(me > 0)
        def _():
            run(False)

        @pl.when(me < n_dev - 1)
        def _():
            for k in range(SWEEPS):
                boundary(k).wait_send()

        @pl.when(me > 0)
        def _():
            for i, name in enumerate("xuldf"):
                ghost_copy(i, name).wait_send()

    ext = n_rows + GHOST
    dma = pltpu.SemaphoreType.DMA

    def vmem(dtype, *shape):
        return pltpu.VMEM(shape, dtype)

    return pl.pallas_call(
        kernel,
        out_shape=pltpu.VMEM((n_rows, size, cols), F32),
        in_specs=[pl.BlockSpec(memory_space=pltpu.HBM)] * 5,
        out_specs=pl.BlockSpec(memory_space=pltpu.VMEM),
        scratch_shapes=[
            vmem(BF16, ext, 2 * size, size), vmem(BF16, ext, size, size),
            vmem(F32, ext, size, cols), vmem(F32, ext + 1, size, cols),
            vmem(F32, ext, cols, size), vmem(BF16, ext + 1, cols, size),
            vmem(BF16, RING, 2 * size, size), vmem(BF16, RING, size, size), vmem(F32, RING, cols, size),
            vmem(F32, 4, cols, size), vmem(BF16, SWEEPS, cols, size), vmem(BF16, SWEEPS, cols, size),
            *[dma((ghost + 1,)) for _ in range(5)], dma((5,)), dma((SWEEPS,)), dma((SWEEPS,)),
        ],
        compiler_params=pltpu.CompilerParams(collective_id=0, has_side_effects=True, vmem_limit_bytes=58_000_000),
    )


def solution(mesh):
    mat_spec = P(("batch", "row"), None, None)
    vec_spec = P(("batch", "row"), None, "col")
    n_dev = mesh.shape["row"]

    def device_fn(d_inv, l_blk, u_blk, rhs_blk, x_init):
        return make_kernel(n_dev, *rhs_blk.shape)(d_inv, l_blk, u_blk, rhs_blk, x_init)

    return jax.shard_map(device_fn, mesh=mesh, in_specs=(mat_spec, mat_spec, mat_spec, vec_spec, vec_spec), out_specs=vec_spec, check_vma=False)
```

```python
import jax
import jax.numpy as jnp
from jax import lax
from jax.experimental import pallas as pl
from jax.experimental.pallas import tpu as pltpu
from jax.sharding import PartitionSpec as P

SWEEPS = 4
GHOST = SWEEPS - 1
LEAD = 2 * SWEEPS - 1
LEAD_FIRST = LEAD + 10
TRIP_FIRST = 10
TRIP = 40
RING = 10
CHUNKS = (1, 1, 2, 4, 4, 6)
EARLY = 4
MESH = pl.DeviceIdType.MESH
BF16, F32 = jnp.bfloat16, jnp.float32
NAMES = "uxdfl"


def dot(a, b):
    return jnp.dot(a, b, preferred_element_type=F32)


def make_kernel(n_dev, n_rows, size, cols):
    last_row = n_rows - 1
    end = n_rows + LEAD
    sizes = list(CHUNKS) + [TRIP_FIRST] * ((n_rows - sum(CHUNKS)) // TRIP_FIRST)
    starts = [sum(sizes[:i]) for i in range(len(sizes))]
    assert sum(sizes) == n_rows and sum(CHUNKS) == LEAD_FIRST + 1 and TRIP_FIRST % RING == 0
    ghost = len(sizes)
    trips_first = ghost - len(CHUNKS)
    trips = (n_rows - 1 - LEAD) // TRIP

    def kernel(d_hbm, l_hbm, u_hbm, f_hbm, x_hbm, out,
               ul_all, d_all, f_raw, x_raw, f_all, x_all, ul_ring, d_ring, f_ring, hold, recv, send,
               sem_l, sem_d, sem_u, sem_f, sem_x, sem_g, sem_s, sem_r):
        me = lax.axis_index("row")
        hbm = {"l": l_hbm, "d": d_hbm, "u": u_hbm, "f": f_hbm, "x": x_hbm}
        sems = {"l": sem_l, "d": sem_d, "u": sem_u, "f": sem_f, "x": sem_x}
        half = {"u": pl.ds(0, size), "l": pl.ds(size, size)}

        def landing(name, rows):
            if name in half:
                return ul_all.at[rows, half[name]]
            return {"d": d_all, "f": f_raw, "x": x_raw}[name].at[rows]

        def local(name, c, start, n):
            if name == "x":
                start = start + 1
            rows = pl.ds(start, n)
            return pltpu.make_async_copy(hbm[name].at[rows], landing(name, rows), sems[name].at[c])

        def chunk(name, c):
            last = name == "x" and c == ghost - 1
            return local(name, c, starts[c], sizes[c] - last)

        for c in range(EARLY):
            for name in NAMES:
                chunk(name, c).start()

        @pl.when(me > 0)
        def _():
            for c in range(EARLY, ghost):
                for name in NAMES:
                    chunk(name, c).start()

        def ghost_rows(name):
            return GHOST + 1 if name == "x" else GHOST

        def ghost_copy(i, name):
            n = ghost_rows(name)
            return pltpu.make_async_remote_copy(
                src_ref=hbm[name].at[pl.ds(0, n)], dst_ref=landing(name, pl.ds(n_rows, n)), send_sem=sem_g.at[i],
                recv_sem=sems[name].at[ghost], device_id={"row": me - 1}, device_id_type=MESH)

        def ghost_local(name):
            n = ghost_rows(name)
            return pltpu.make_async_copy(
                hbm[name].at[pl.ds(0, n)], landing(name, pl.ds(n_rows, n)), sems[name].at[ghost])

        def ghost_wait(name):
            ghost_local(name).wait()

        barrier = pltpu.get_barrier_semaphore()

        @pl.when(me > 0)
        def _():
            pl.semaphore_signal(barrier, inc=1, device_id={"row": me - 1}, device_id_type=MESH)

        @pl.when(me < n_dev - 1)
        def _():
            pl.semaphore_signal(barrier, inc=1, device_id={"row": me + 1}, device_id_type=MESH)

        pl.semaphore_wait(barrier, jnp.where(me > 0, 1, 0) + jnp.where(me < n_dev - 1, 1, 0))

        @pl.when(me > 0)
        def _():
            for i, name in enumerate("xuldf"):
                ghost_copy(i, name).start()

        @pl.when(me == n_dev - 1)
        def _():
            for name in "xuldf":
                ghost_local(name).start()

        def boundary(k):
            return pltpu.make_async_remote_copy(
                src_ref=send.at[k], dst_ref=recv.at[k], send_sem=sem_s.at[k], recv_sem=sem_r.at[k],
                device_id={"row": me + 1}, device_id_type=MESH)

        def run(ring):
            lead = LEAD_FIRST if ring else LEAD
            per_trip, n_trips = (TRIP_FIRST, trips_first) if ring else (TRIP, trips)
            main_end = lead + per_trip * n_trips
            ul, d, f = (ul_ring, d_ring, f_ring) if ring else (ul_all, d_all, f_all)

            def where(base, p):
                return p if base is None else base + (p - lead)

            def slot(base, r):
                return r % RING if ring else where(base, r)

            def prep_one(name, base, r):
                at, to = where(base, r), slot(base, r)
                if name in half:
                    ul[to, half[name]] = ul_all[at, half[name]].T
                elif name == "d":
                    d[to] = d_all[at].T
                elif name == "f":
                    f[to] = f_raw[at].T
                else:
                    x_all[at + 1] = x_raw[at + 1].astype(BF16).T

            def prep(base, r):
                for name in "uldfx":
                    prep_one(name, base, r)

            def active(k, s):
                return 0 <= s - 2 * (k - 1) <= last_row + SWEEPS - k

            def period(live, p, base=None, row=None):
                x = {}
                left = [] if row is None else list("uldxf")

                def fill():
                    if left:
                        prep_one(left.pop(0), base, row)

                def get_x(k):
                    if ("x", k) in live:
                        val = live.pop(("x", k))
                        x[k] = val.astype(BF16)
                        if k == SWEEPS and ring:
                            f_all[where(base, p - LEAD)] = val
                        elif k == SWEEPS:
                            out[where(base, p - LEAD)] = val.T
                        if base is None and p - 1 - 2 * (k - 1) == last_row:
                            send[k - 1] = x[k]

                            @pl.when(me < n_dev - 1)
                            def _():
                                boundary(k - 1).start()
                    elif base is None and p == 2 * (k - 1) and not ring:
                        boundary(k - 1).wait_recv()
                        x[k] = recv[k - 1]

                def sums(k):
                    get_x(k)
                    if not active(k, p):
                        return
                    r = p - 2 * (k - 1)
                    right = x_all[where(base, r + 1)] if k == 1 else x[k - 1]
                    if base is None and k > 1 and r == last_row:
                        right = jnp.where(me < n_dev - 1, right, jnp.zeros_like(right))
                    if k in x:
                        live["t", k] = dot(jnp.concatenate([right, x[k]], axis=1), ul[slot(base, r)])
                    else:
                        live["t", k] = dot(right, ul[slot(base, r), half["u"]])

                def solve(k, s):
                    if ("t", k) in live:
                        to = slot(base, s - 2 * (k - 1))
                        live["x", k] = dot((f[to] - live.pop(("t", k))).astype(BF16), d[to])

                fill()
                sums(1)
                sums(2)
                fill()
                solve(3, p - 1)
                sums(3)
                fill()
                solve(4, p - 1)
                solve(1, p)
                fill()
                sums(4)
                solve(2, p)
                fill()

            carried = (("x", 1), ("x", 2), ("t", 3), ("t", 4))

            def keep(live):
                for i, key in enumerate(carried):
                    hold[i] = live[key]

            def load():
                return {key: hold[i] for i, key in enumerate(carried)}

            if ring:
                waited = set()

                def need(r):
                    c = max(i for i, start in enumerate(starts) if start <= r)
                    if c not in waited:
                        waited.add(c)
                        for name in NAMES:
                            chunk(name, c).wait()

                need(0)
                prep(None, 0)
            else:
                for c in range(1, ghost):
                    for i in ([0, 1] if c == 1 else [c]):
                        for name in NAMES:
                            chunk(name, i).wait()
                    if c == ghost - 1:
                        ghost_wait("x")
                    start = 0 if c == 1 else starts[c]

                    def pair(i, carry, start=start):
                        prep(start + 2 * i, lead)
                        prep(start + 2 * i, lead + 1)
                        return carry
                    lax.fori_loop(0, (starts[c] + sizes[c] - start) // 2, pair, 0)
            live = {}
            for p in range(lead):
                if ring and p % 2 and EARLY + p // 2 < ghost:
                    for name in NAMES:
                        chunk(name, EARLY + p // 2).start()
                if ring:
                    need(p + 1)
                period(live, p, None, p + 1 if ring else None)
            keep(live)

            def trip(b, carry):
                base = lead + per_trip * b
                if ring:
                    c, start = len(CHUNKS) + b, lead + 1 + per_trip * b
                    for name in "udfl":
                        local(name, c, start, per_trip).wait()

                    @pl.when(b < n_trips - 1)
                    def _():
                        local("x", c, start, per_trip).wait()

                    @pl.when(b == n_trips - 1)
                    def _():
                        chunk("x", ghost - 1).wait()
                        ghost_wait("x")
                live = load()
                for p in range(lead, lead + per_trip):
                    period(live, p, base, p + 1 if ring else None)
                keep(live)
                return carry
            lax.fori_loop(0, n_trips, trip, 0)

            for name in "uldf":
                ghost_wait(name)
            live = load()
            for p in range(main_end, end):
                period(live, p, None, p + 1 if n_rows <= p + 1 < n_rows + GHOST else None)
            if ring:
                def turn(i, carry):
                    for j in range(2):
                        out[2 * i + j] = f_all[2 * i + j].T
                    return carry
                lax.fori_loop(0, n_rows // 2, turn, 0)

        @pl.when(me == 0)
        def _():
            run(True)

        @pl.when(me > 0)
        def _():
            run(False)

        @pl.when(me < n_dev - 1)
        def _():
            for k in range(SWEEPS):
                boundary(k).wait_send()

        @pl.when(me > 0)
        def _():
            for i, name in enumerate("xuldf"):
                ghost_copy(i, name).wait_send()

    ext = n_rows + GHOST
    dma = pltpu.SemaphoreType.DMA

    def vmem(dtype, *shape):
        return pltpu.VMEM(shape, dtype)

    return pl.pallas_call(
        kernel,
        out_shape=pltpu.VMEM((n_rows, size, cols), F32),
        in_specs=[pl.BlockSpec(memory_space=pltpu.HBM)] * 5,
        out_specs=pl.BlockSpec(memory_space=pltpu.VMEM),
        scratch_shapes=[
            vmem(BF16, ext, 2 * size, size), vmem(BF16, ext, size, size),
            vmem(F32, ext, size, cols), vmem(F32, ext + 1, size, cols),
            vmem(F32, ext, cols, size), vmem(BF16, ext + 1, cols, size),
            vmem(BF16, RING, 2 * size, size), vmem(BF16, RING, size, size), vmem(F32, RING, cols, size),
            vmem(F32, 4, cols, size), vmem(BF16, SWEEPS, cols, size), vmem(BF16, SWEEPS, cols, size),
            *[dma((ghost + 1,)) for _ in range(5)], dma((5,)), dma((SWEEPS,)), dma((SWEEPS,)),
        ],
        compiler_params=pltpu.CompilerParams(collective_id=0, has_side_effects=True, vmem_limit_bytes=58_000_000),
    )


def solution(mesh):
    mat_spec = P(("batch", "row"), None, None)
    vec_spec = P(("batch", "row"), None, "col")
    n_dev = mesh.shape["row"]

    def device_fn(d_inv, l_blk, u_blk, rhs_blk, x_init):
        return make_kernel(n_dev, *rhs_blk.shape)(d_inv, l_blk, u_blk, rhs_blk, x_init)

    return jax.shard_map(device_fn, mesh=mesh, in_specs=(mat_spec, mat_spec, mat_spec, vec_spec, vec_spec), out_specs=vec_spec, check_vma=False)
```

```python
import jax
import jax.numpy as jnp
from jax import lax
from jax.experimental import pallas as pl
from jax.experimental.pallas import tpu as pltpu
from jax.sharding import PartitionSpec as P

SWEEPS = 4
GHOST = SWEEPS - 1
LEAD = 2 * SWEEPS - 1
LEAD_FIRST = LEAD + 10
TRIP_FIRST = 10
TRIP = 40
RING = 10
CHUNKS = (1, 1, 2, 4, 4, 6)
EARLY = 4
MESH = pl.DeviceIdType.MESH
BF16, F32 = jnp.bfloat16, jnp.float32
NAMES = "uxdfl"


def dot(a, b):
    return jnp.dot(a, b, preferred_element_type=F32)


def make_kernel(n_dev, n_rows, size, cols):
    last_row = n_rows - 1
    end = n_rows + LEAD
    sizes = list(CHUNKS) + [TRIP_FIRST] * ((n_rows - sum(CHUNKS)) // TRIP_FIRST)
    starts = [sum(sizes[:i]) for i in range(len(sizes))]
    assert sum(sizes) == n_rows and sum(CHUNKS) == LEAD_FIRST + 1 and TRIP_FIRST % RING == 0
    ghost = len(sizes)
    trips_first = ghost - len(CHUNKS)
    trips = (n_rows - 1 - LEAD) // TRIP

    def kernel(d_hbm, l_hbm, u_hbm, f_hbm, x_hbm, out,
               ul_all, d_all, f_raw, x_raw, f_all, x_all, ul_ring, d_ring, f_ring, hold, recv, send,
               sem_l, sem_d, sem_u, sem_f, sem_x, sem_g, sem_s, sem_r):
        me = lax.axis_index("row")
        hbm = {"l": l_hbm, "d": d_hbm, "u": u_hbm, "f": f_hbm, "x": x_hbm}
        sems = {"l": sem_l, "d": sem_d, "u": sem_u, "f": sem_f, "x": sem_x}
        half = {"u": pl.ds(0, size), "l": pl.ds(size, size)}

        def landing(name, rows):
            if name in half:
                return ul_all.at[rows, half[name]]
            return {"d": d_all, "f": f_raw, "x": x_raw}[name].at[rows]

        def local(name, c, start, n):
            if name == "x":
                start = start + 1
            rows = pl.ds(start, n)
            return pltpu.make_async_copy(hbm[name].at[rows], landing(name, rows), sems[name].at[c])

        def chunk(name, c):
            last = name == "x" and c == ghost - 1
            return local(name, c, starts[c], sizes[c] - last)

        for c in range(EARLY):
            for name in NAMES:
                chunk(name, c).start()

        @pl.when(me > 0)
        def _():
            for c in range(EARLY, ghost):
                for name in NAMES:
                    chunk(name, c).start()

        def ghost_rows(name):
            return GHOST + 1 if name == "x" else GHOST

        def ghost_copy(i, name):
            n = ghost_rows(name)
            return pltpu.make_async_remote_copy(
                src_ref=hbm[name].at[pl.ds(0, n)], dst_ref=landing(name, pl.ds(n_rows, n)), send_sem=sem_g.at[i],
                recv_sem=sems[name].at[ghost], device_id={"row": me - 1}, device_id_type=MESH)

        def ghost_local(name):
            n = ghost_rows(name)
            return pltpu.make_async_copy(
                hbm[name].at[pl.ds(0, n)], landing(name, pl.ds(n_rows, n)), sems[name].at[ghost])

        def ghost_wait(name):
            ghost_local(name).wait()

        barrier = pltpu.get_barrier_semaphore()

        @pl.when(me > 0)
        def _():
            pl.semaphore_signal(barrier, inc=1, device_id={"row": me - 1}, device_id_type=MESH)

        @pl.when(me < n_dev - 1)
        def _():
            pl.semaphore_signal(barrier, inc=1, device_id={"row": me + 1}, device_id_type=MESH)

        pl.semaphore_wait(barrier, jnp.where(me > 0, 1, 0) + jnp.where(me < n_dev - 1, 1, 0))

        @pl.when(me > 0)
        def _():
            for i, name in enumerate("xuldf"):
                ghost_copy(i, name).start()

        @pl.when(me == n_dev - 1)
        def _():
            for name in "xuldf":
                ghost_local(name).start()

        def boundary(k):
            return pltpu.make_async_remote_copy(
                src_ref=send.at[k], dst_ref=recv.at[k], send_sem=sem_s.at[k], recv_sem=sem_r.at[k],
                device_id={"row": me + 1}, device_id_type=MESH)

        def run(ring):
            lead = LEAD_FIRST if ring else LEAD
            per_trip, n_trips = (TRIP_FIRST, trips_first) if ring else (TRIP, trips)
            main_end = lead + per_trip * n_trips
            ul, d, f = (ul_ring, d_ring, f_ring) if ring else (ul_all, d_all, f_all)

            def where(base, p):
                return p if base is None else base + (p - lead)

            def slot(base, r):
                return r % RING if ring else where(base, r)

            def prep_one(name, base, r):
                at, to = where(base, r), slot(base, r)
                if name in half:
                    ul[to, half[name]] = ul_all[at, half[name]].T
                elif name == "d":
                    d[to] = d_all[at].T
                elif name == "f":
                    f[to] = f_raw[at].T
                else:
                    x_all[at + 1] = x_raw[at + 1].astype(BF16).T

            def prep(base, r):
                for name in "uldfx":
                    prep_one(name, base, r)

            def active(k, s):
                return 0 <= s - 2 * (k - 1) <= last_row + SWEEPS - k

            def period(live, p, base=None, row=None):
                x = {}
                left = [] if row is None else list("uldxf")

                def fill():
                    if left:
                        prep_one(left.pop(0), base, row)

                def get_x(k):
                    if ("x", k) in live:
                        val = live.pop(("x", k))
                        x[k] = val.astype(BF16)
                        if k == SWEEPS and ring:
                            f_all[where(base, p - LEAD)] = val
                        elif k == SWEEPS:
                            out[where(base, p - LEAD)] = val.T
                        if base is None and p - 1 - 2 * (k - 1) == last_row:
                            send[k - 1] = x[k]

                            @pl.when(me < n_dev - 1)
                            def _():
                                boundary(k - 1).start()
                    elif base is None and p == 2 * (k - 1) and not ring:
                        boundary(k - 1).wait_recv()
                        x[k] = recv[k - 1]

                def sums(k):
                    get_x(k)
                    if not active(k, p):
                        return
                    r = p - 2 * (k - 1)
                    right = x_all[where(base, r + 1)] if k == 1 else x[k - 1]
                    if base is None and k > 1 and r == last_row:
                        right = jnp.where(me < n_dev - 1, right, jnp.zeros_like(right))
                    if k in x:
                        live["t", k] = dot(jnp.concatenate([right, x[k]], axis=1), ul[slot(base, r)])
                    else:
                        live["t", k] = dot(right, ul[slot(base, r), half["u"]])

                def solve(k, s):
                    if ("t", k) in live:
                        to = slot(base, s - 2 * (k - 1))
                        live["x", k] = dot((f[to] - live.pop(("t", k))).astype(BF16), d[to])

                fill()
                solve(3, p - 1)
                sums(1)
                sums(2)
                fill()
                sums(3)
                fill()
                solve(4, p - 1)
                solve(1, p)
                fill()
                sums(4)
                solve(2, p)
                fill()

            carried = (("x", 1), ("x", 2), ("t", 3), ("t", 4))

            def keep(live):
                for i, key in enumerate(carried):
                    hold[i] = live[key]

            def load():
                return {key: hold[i] for i, key in enumerate(carried)}

            if ring:
                waited = set()

                def need(r):
                    c = max(i for i, start in enumerate(starts) if start <= r)
                    if c not in waited:
                        waited.add(c)
                        for name in NAMES:
                            chunk(name, c).wait()

                need(0)
                prep(None, 0)
            else:
                for c in range(1, ghost):
                    for i in ([0, 1] if c == 1 else [c]):
                        for name in NAMES:
                            chunk(name, i).wait()
                    if c == ghost - 1:
                        ghost_wait("x")
                    start = 0 if c == 1 else starts[c]

                    def pair(i, carry, start=start):
                        prep(start + 2 * i, lead)
                        prep(start + 2 * i, lead + 1)
                        return carry
                    lax.fori_loop(0, (starts[c] + sizes[c] - start) // 2, pair, 0)
            live = {}
            for p in range(lead):
                if ring and p % 2 and EARLY + p // 2 < ghost:
                    for name in NAMES:
                        chunk(name, EARLY + p // 2).start()
                if ring:
                    need(p + 1)
                period(live, p, None, p + 1 if ring else None)
            def trip(b, carry):
                base = lead + per_trip * b
                if ring:
                    c, start = len(CHUNKS) + b, lead + 1 + per_trip * b
                    for name in "udfl":
                        local(name, c, start, per_trip).wait()

                    @pl.when(b < n_trips - 1)
                    def _():
                        local("x", c, start, per_trip).wait()

                    @pl.when(b == n_trips - 1)
                    def _():
                        chunk("x", ghost - 1).wait()
                        ghost_wait("x")
                live = load()
                for p in range(lead, lead + per_trip):
                    period(live, p, base, p + 1 if ring else None)
                keep(live)
                return carry
            if ring:
                keep(live)
                lax.fori_loop(0, n_trips, trip, 0)
                live = load()
            else:
                for p in range(lead, main_end):
                    period(live, p)

            for name in "uldf":
                ghost_wait(name)
            for p in range(main_end, end):
                period(live, p, None, p + 1 if n_rows <= p + 1 < n_rows + GHOST else None)
            if ring:
                def turn(i, carry):
                    for j in range(2):
                        out[2 * i + j] = f_all[2 * i + j].T
                    return carry
                lax.fori_loop(0, n_rows // 2, turn, 0)

        @pl.when(me == 0)
        def _():
            run(True)

        @pl.when(me > 0)
        def _():
            run(False)

        @pl.when(me < n_dev - 1)
        def _():
            for k in range(SWEEPS):
                boundary(k).wait_send()

        @pl.when(me > 0)
        def _():
            for i, name in enumerate("xuldf"):
                ghost_copy(i, name).wait_send()

    ext = n_rows + GHOST
    dma = pltpu.SemaphoreType.DMA

    def vmem(dtype, *shape):
        return pltpu.VMEM(shape, dtype)

    return pl.pallas_call(
        kernel,
        out_shape=pltpu.VMEM((n_rows, size, cols), F32),
        in_specs=[pl.BlockSpec(memory_space=pltpu.HBM)] * 5,
        out_specs=pl.BlockSpec(memory_space=pltpu.VMEM),
        scratch_shapes=[
            vmem(BF16, ext, 2 * size, size), vmem(BF16, ext, size, size),
            vmem(F32, ext, size, cols), vmem(F32, ext + 1, size, cols),
            vmem(F32, ext, cols, size), vmem(BF16, ext + 1, cols, size),
            vmem(BF16, RING, 2 * size, size), vmem(BF16, RING, size, size), vmem(F32, RING, cols, size),
            vmem(F32, 4, cols, size), vmem(BF16, SWEEPS, cols, size), vmem(BF16, SWEEPS, cols, size),
            *[dma((ghost + 1,)) for _ in range(5)], dma((5,)), dma((SWEEPS,)), dma((SWEEPS,)),
        ],
        compiler_params=pltpu.CompilerParams(collective_id=0, has_side_effects=True, vmem_limit_bytes=58_000_000),
    )


def solution(mesh):
    mat_spec = P(("batch", "row"), None, None)
    vec_spec = P(("batch", "row"), None, "col")
    n_dev = mesh.shape["row"]

    def device_fn(d_inv, l_blk, u_blk, rhs_blk, x_init):
        return make_kernel(n_dev, *rhs_blk.shape)(d_inv, l_blk, u_blk, rhs_blk, x_init)

    return jax.shard_map(device_fn, mesh=mesh, in_specs=(mat_spec, mat_spec, mat_spec, vec_spec, vec_spec), out_specs=vec_spec, check_vma=False)
```
